32 devices in a mesh: dp: 4 (over z), sp: 8 (over y, x, core).
Axes of the slice: x: 2, y: 2, z: 4, core: 2. Of those that a mesh axis runs over, the one named last changes fastest.
Arguments:
- queries_in: bfloat16 [8, 8192, 16, 128], P('dp', 'sp'), may hold values from -6 to 6
- keys_in: bfloat16 [8, 8192, 16, 128], P('dp', 'sp'), may hold values from -6 to 6
- values_in: bfloat16 [8, 8192, 16, 128], P('dp', 'sp'), may hold values from -6 to 6
- out_weight: bfloat16 [2048, 2048], P('dp'), may hold values from -0.125 to 0.125
Outputs:
- block_out: bfloat16 [8, 8192, 2048], P('dp', 'sp')
The draws below stay inside these ranges and needn't reach their ends.
All inputs are finite; a program needn't handle non-finite values.
Results may differ from the reference program's by a relative error of at most 0.006.
Values may be sent and summed in bfloat16 or wider, within the bound.
A program may use at most 320 MiB of HBM per device.

```python
import jax
import jax.numpy as jnp
from jax import lax

HEADS = 16
HEAD_SIZE = 128
BATCH = 8
TOKENS = 8192
WIDTH = 2048


def block_levels(own_key, dims, cuts, least, top_value):
    def one(dim, shards_of):
        draws = jax.random.uniform(jax.random.fold_in(jax.random.fold_in(own_key, 6), dim), (shards_of,), jnp.float32, least / len(cuts), top_value / len(cuts))
        return jnp.repeat(jnp.exp(draws), dims[dim] // shards_of).reshape((-1,) + (1,) * (len(dims) - dim - 1))

    gain = one(*cuts[0])
    for cut in cuts[1:]:
        gain = gain * one(*cut)
    return gain


def bell_draw(key, extent, deviation, limit, cuts=(), kind=jnp.bfloat16):
    loudness = block_levels(key, extent, cuts, -0.22, 0.18) if cuts else 1.0
    drawn = jax.random.normal(key, extent, jnp.float32) * deviation * loudness
    return jnp.minimum(jnp.maximum(drawn, -limit), limit).astype(kind)


def setup_inputs(seed: int = 0) -> dict:
    key_list = jax.random.split(jax.random.key(seed), 5)
    queries_in = bell_draw(key_list[0], (BATCH, TOKENS, HEADS, HEAD_SIZE), 1.0, 6.0, ((0, 4), (1, 8)))
    keys_in = bell_draw(key_list[1], (BATCH, TOKENS, HEADS, HEAD_SIZE), 1.0, 6.0, ((0, 4), (1, 8)))
    values_in = bell_draw(key_list[2], (BATCH, TOKENS, HEADS, HEAD_SIZE), 1.0, 6.0, ((0, 4), (1, 8)))
    out_weight = bell_draw(key_list[3], (WIDTH, WIDTH), WIDTH ** -0.5, 0.125, ((0, 4),))
    return dict(queries_in=queries_in, keys_in=keys_in, values_in=values_in, out_weight=out_weight)


def feature_map(values):
    wide = values.astype(jnp.float32)
    return (wide * wide + 0.1).astype(jnp.bfloat16)


def finish_heads(read, count):
    result = read * count ** 0.5
    return result.astype(jnp.bfloat16)


def look_up(features, state, mass):
    small = lax.optimization_barrier(state.astype(jnp.bfloat16))
    top = jnp.einsum("bthd,bhde->bthe", features.astype(jnp.float32), small.astype(jnp.float32))
    bottom = jnp.einsum("bthd,bhd->bth", features.astype(jnp.float32), mass, precision=lax.Precision.HIGHEST)
    return top / (bottom + 1e-3)[..., None]


def reference(queries_in, keys_in, values_in, out_weight):
    query_feature, key_feature = lax.optimization_barrier((feature_map(queries_in), feature_map(keys_in)))
    state = jnp.einsum("bthd,bthe->bhde", key_feature.astype(jnp.float32), values_in.astype(jnp.float32)) / TOKENS
    mass = jnp.sum(key_feature.astype(jnp.float32), axis=1) / TOKENS
    mixed = finish_heads(look_up(query_feature, state, mass), TOKENS).reshape(BATCH, TOKENS, WIDTH)
    mixed = lax.optimization_barrier(mixed)
    block_out = jnp.einsum("btw,wv->btv", mixed.astype(jnp.float32), out_weight.astype(jnp.float32)).astype(jnp.bfloat16)
    return block_out
```

```python
import functools

import jax
import jax.numpy as jnp
from jax import lax
from jax.experimental import pallas as pl
from jax.experimental.pallas import tpu as pltpu
from jax.sharding import PartitionSpec as P

MESH = pl.DeviceIdType.MESH
SLOTS = 3
TILE = 256
PITCH = 24
EXTRA = 16


def feature_map(values):
    wide = values.astype(jnp.float32)
    return wide * wide + 0.1


def split_mass(mass):
    high = mass.astype(jnp.bfloat16).astype(jnp.float32)
    row = lax.broadcasted_iota(jnp.int32, mass.shape, mass.ndim - 2)
    return jnp.where(row % 2 == 0, high, mass - high).astype(jnp.bfloat16)


def gather_kernel(
    groups, count, tile, batch, tokens, heads, size,
    q_ref, k_ref, v_ref, w_ref, mixed_ref, wide_ref,
    k_buf, v_buf, q_buf, mixed_buf, rel_k, rel_v, total, core_in, out_buf, in_buf,
    final, table, w_all,
    load_sem, q_sem, mixed_sem, own_sem, wide_sem,
    z_send, z_recv, n_send, n_recv, p_send, p_recv, m_send, m_recv,
    c_send, c_recv, r_send, r_recv, g_send, g_recv, f_send, f_recv,
):
    f32, bf16 = jnp.float32, jnp.bfloat16
    depth, lanes = groups
    places = lanes // 2
    levels = places.bit_length() - 1
    d, s = lax.axis_index("dp"), lax.axis_index("sp")
    core, place = s % 2, s // 2
    rows, width = w_ref.shape
    part, half_width = rows // 4, width // 2
    per_batch = tokens // tile
    steps = batch * per_batch
    held = heads // 2
    piece = held // places
    root = count**0.5

    def flip(value, bit):
        return value + (1 << bit) - 2 * (1 << bit) * ((value // (1 << bit)) % 2)

    def peer_place(k):
        other = place
        for bit in range(levels):
            if k >> bit & 1:
                other = flip(other, bit)
        return other

    partner = {"sp": flip(s, 0)}
    peers = [{"sp": 2 * peer_place(k) + core} for k in range(1, places)]
    sides = [{"sp": flip(s, 1)}, {"sp": flip(s, levels)}]
    parity = place % 2
    if levels > 1:
        parity = (parity + (place // (1 << (levels - 1))) % 2) % 2
    quarter, across = parity * 2 + core, (1 - parity) * 2 + core

    barrier = pltpu.get_barrier_semaphore()
    for device in [partner] + peers + [{"dp": (d + k) % depth} for k in (1, depth - 1)]:
        pl.semaphore_signal(barrier, inc=1, device_id=device, device_id_type=MESH)

    def load(i):
        b, t, slot = i // per_batch, i % per_batch, i % SLOTS
        at = pl.ds(t * tile, tile)
        return (
            pltpu.make_async_copy(k_ref.at[b, at], k_buf.at[slot], load_sem.at[0, slot]),
            pltpu.make_async_copy(v_ref.at[b, at], v_buf.at[slot], load_sem.at[1, slot]),
        )

    def load_q(i):
        b, t, slot = i // per_batch, i % per_batch, i % SLOTS
        return pltpu.make_async_copy(
            q_ref.at[b, pl.ds(t * tile, tile)], q_buf.at[slot], q_sem.at[slot]
        )

    def store_mixed(i):
        return pltpu.make_async_copy(
            mixed_buf.at[i % 2], mixed_ref.at[pl.ds(i * tile, tile)], mixed_sem.at[i % 2]
        )

    for i in range(min(SLOTS - 1, steps)):
        for copy in load(i):
            copy.start()
    own = pltpu.make_async_copy(w_ref, w_all.at[d], own_sem)
    own.start()
    total[...] = jnp.zeros_like(total)
    table[...] = jnp.zeros_like(table)
    pl.semaphore_wait(barrier, places + 2)

    def origin(way, hop):
        return d - hop if way == 0 else d + hop

    def inside(place_on_dp):
        return jnp.logical_and(place_on_dp >= 0, place_on_dp < depth)

    def sends(way, hop):
        return jnp.logical_and(inside(origin(way, hop - 1)), inside(origin(way, -1)))

    def block(from_dp, index, side):
        return w_all.at[
            from_dp, pl.ds(index * part, part), pl.ds(side * half_width, half_width)
        ]

    def z_copy(way, hop, side):
        target = block(origin(way, hop - 1), quarter, side)
        source = target
        if hop == 1:
            source = w_ref.at[
                pl.ds(quarter * part, part), pl.ds(side * half_width, half_width)
            ]
        return pltpu.make_async_remote_copy(
            src_ref=source, dst_ref=target,
            send_sem=z_send.at[way, hop, side], recv_sem=z_recv.at[way, hop, side],
            device_id={"dp": (d + (1 if way == 0 else depth - 1)) % depth},
            device_id_type=MESH,
        )

    def z_arrival(way, hop, side):
        target = block(origin(way, hop), quarter, side)
        return pltpu.make_async_remote_copy(
            src_ref=target, dst_ref=target,
            send_sem=z_send.at[way, hop, side], recv_sem=z_recv.at[way, hop, side],
            device_id={"dp": (d + 1) % depth}, device_id_type=MESH,
        )

    def spread(way, hop, side, index, send, recv, device):
        target = block(origin(way, hop), index, side)
        return pltpu.make_async_remote_copy(
            src_ref=target, dst_ref=target,
            send_sem=send.at[way, hop, side], recv_sem=recv.at[way, hop, side],
            device_id=device, device_id_type=MESH,
        )

    def n_copy(way, hop, side):
        return spread(way, hop, side, quarter, n_send, n_recv, sides[side])

    def p_copy(way, hop, side):
        return spread(way, hop, side, quarter, p_send, p_recv, partner)

    def m_copy(way, hop, side):
        return spread(way, hop, side, across, m_send, m_recv, partner)

    def each_way(hop, act):
        for way in range(2):
            pl.when(inside(origin(way, hop)))(functools.partial(act, way))

    def z_event(hop, side):
        each_way(hop, lambda way: z_arrival(way, hop, side).wait_recv())
        if hop + 1 < depth:
            for way in range(2):
                pl.when(sends(way, hop + 1))(
                    lambda way=way: z_copy(way, hop + 1, side).start()
                )

        def forward(way):
            n_copy(way, hop, side).start()
            p_copy(way, hop, side).start()

        each_way(hop, forward)

    def n_event(hop, side):
        def act(way):
            n_copy(way, hop, side).wait_recv()
            m_copy(way, hop, side).start()

        each_way(hop, act)

    def wide_copy(way, hop):
        at = origin(way, hop)
        return pltpu.make_async_copy(
            w_all.at[at], wide_ref.at[pl.ds(at * rows, rows)], wide_sem.at[way, hop]
        )

    def f_event(hop):
        def act(way):
            for side in range(2):
                p_copy(way, hop, side).wait_recv()
                m_copy(way, hop, side).wait_recv()
            wide_copy(way, hop).start()

        each_way(hop, act)

    def w_end():
        for hop in range(1, depth):
            for way in range(2):
                for side in range(2):
                    pl.when(sends(way, hop))(
                        lambda way=way, hop=hop, side=side: z_copy(way, hop, side).wait_send()
                    )

            def act(way, hop=hop):
                for side in range(2):
                    for make in (n_copy, p_copy, m_copy):
                        make(way, hop, side).wait_send()
                wide_copy(way, hop).wait()

            each_way(hop, act)
        own_out.wait()

    for side in range(2):
        for way in range(2):
            pl.when(sends(way, 1))(lambda way=way, side=side: z_copy(way, 1, side).start())

    def c_copy(b):
        return pltpu.make_async_remote_copy(
            src_ref=total.at[b, pl.ds((1 - core) * held, held)], dst_ref=core_in.at[b],
            send_sem=c_send.at[b], recv_sem=c_recv.at[b],
            device_id=partner, device_id_type=MESH,
        )

    def r_copy(b, k):
        return pltpu.make_async_remote_copy(
            src_ref=out_buf.at[b, pl.ds(peer_place(k) * piece, piece)],
            dst_ref=in_buf.at[b, k - 1],
            send_sem=r_send.at[b, k], recv_sem=r_recv.at[b, k],
            device_id=peers[k - 1], device_id_type=MESH,
        )

    def g_copy(b, k):
        at = final.at[b, pl.ds(core * held + place * piece, piece)]
        return pltpu.make_async_remote_copy(
            src_ref=at, dst_ref=at, send_sem=g_send.at[b, k], recv_sem=g_recv.at[b, k],
            device_id=peers[k - 1], device_id_type=MESH,
        )

    def f_copy(b):
        at = final.at[b, pl.ds(core * held, held)]
        return pltpu.make_async_remote_copy(
            src_ref=at, dst_ref=at, send_sem=f_send.at[b], recv_sem=f_recv.at[b],
            device_id=partner, device_id_type=MESH,
        )

    def x_add(b):
        c_copy(b).wait()
        mine = pl.ds(core * held, held)
        summed = total[b, mine] + core_in[b]
        total[b, mine] = summed
        out_buf[b, :, :size] = summed[:, :size].astype(bf16)
        out_buf[b, :, size:] = split_mass(summed[:, size:])
        for k in range(1, places):
            r_copy(b, k).start()

    def x_sum(b):
        mine = pl.ds(core * held + place * piece, piece)
        state, mass = total[b, mine, :size], total[b, mine, size:]
        for k in range(1, places):
            r_copy(b, k).wait_recv()
            state += in_buf[b, k - 1, :, :size].astype(f32)
            pair = in_buf[b, k - 1, :, size:].astype(f32)
            mass += pair[:, :1] + pair[:, 1:2]
        final[b, mine, :size] = (state / count).astype(bf16)
        final[b, mine, size:] = split_mass(mass / count / root)
        for k in range(1, places):
            g_copy(b, k).start()

    def x_share(b):
        for k in range(1, places):
            g_copy(b, k).wait_recv()
        f_copy(b).start()

    def x_table(b):
        f_copy(b).wait_recv()
        for h in range(heads):
            pair = final[b, h, size:].astype(f32)
            table[h, :size, :size] = final[b, h, :size]
            table[h, size:, :size] = jnp.broadcast_to(pair[:1], (size, size)).astype(bf16)
            table[h, size:, size:] = jnp.broadcast_to(pair[1:2], (size, size)).astype(bf16)

    def x_end(b):
        for k in range(1, places):
            r_copy(b, k).wait_send()
            g_copy(b, k).wait_send()
        f_copy(b).wait_send()

    def relay(buffer, values):
        buffer.reshape(tile, PITCH, size)[:, :heads, :] = values

    def pick(buffer, h):
        return buffer[pl.ds(h, tile, stride=PITCH), :].astype(bf16)

    ones = jnp.ones((EXTRA, tile), bf16)

    def fold(i):
        slot, b = i % SLOTS, i // per_batch
        relay(rel_k, feature_map(k_buf[slot]))
        relay(rel_v, v_buf[slot].astype(f32))
        for h in range(heads):
            left = jnp.concatenate([jnp.transpose(pick(rel_v, h)), ones], axis=0)
            total[b, h] += jnp.dot(left, pick(rel_k, h), preferred_element_type=f32)

    def read(i):
        relay(rel_k, feature_map(q_buf[i % SLOTS]))
        for h in range(heads):
            feature = pick(rel_k, h)
            both = lax.dot_general(
                jnp.concatenate([feature, feature], axis=1), table[h],
                (((1,), (1,)), ((), ())), preferred_element_type=f32,
            )
            top = both[:, :size] / (both[:, size:] + 0.001 / root)
            mixed_buf[i % 2, :, h * size : (h + 1) * size] = top.astype(bf16)

    def at_step(i, events):
        for moment, items in events.items():
            def run(items=items):
                for item in items:
                    item()

            pl.when(i == moment)(run)

    def make(function, *args):
        return functools.partial(function, *args)

    first = per_batch
    fold_events = {
        first: [lambda: c_copy(0).start(), make(z_event, 1, 0)],
        first + 1: [make(x_add, 0)],
        first + 2: [make(z_event, 1, 1)],
        first + 3: [make(x_sum, 0), make(n_event, 1, 0)],
    }

    def fold_step(i, carry):
        @pl.when(i + SLOTS - 1 < steps)
        def _():
            for copy in load(i + SLOTS - 1):
                copy.start()

        @pl.when(i + SLOTS - 1 >= steps)
        def _():
            load_q(i + SLOTS - 1 - steps).start()

        at_step(i, fold_events)
        for copy in load(i):
            copy.wait()
        fold(i)
        return carry

    lax.fori_loop(0, steps, fold_step, 0)
    own.wait()
    own_out = pltpu.make_async_copy(w_all.at[d], wide_ref.at[pl.ds(d * rows, rows)], own_sem)
    own_out.start()
    c_copy(1).start()
    x_share(0)
    n_event(1, 1)
    z_event(2, 0)
    x_add(1)
    x_table(0)

    last = per_batch
    read_events = {
        1: [make(z_event, 2, 1), make(x_sum, 1), make(n_event, 2, 0)],
        2: [make(f_event, 1), make(z_event, 3, 0)],
        3: [make(x_share, 1), make(n_event, 2, 1)],
        last: [make(x_table, 1), make(z_event, 3, 1)],
        last + 1: [make(n_event, 3, 0), make(f_event, 2)],
        last + 3: [make(n_event, 3, 1)],
    }

    def read_step(i, carry):
        @pl.when(i + SLOTS - 1 < steps)
        def _():
            load_q(i + SLOTS - 1).start()

        at_step(i, read_events)
        load_q(i).wait()
        pl.when(i > 1)(lambda: store_mixed(i - 2).wait())
        read(i)
        store_mixed(i).start()
        return carry

    lax.fori_loop(0, steps, read_step, 0)
    for hop in range(4, depth):
        for side in range(2):
            z_event(hop, side)
        for side in range(2):
            n_event(hop, side)
    for hop in range(3, depth):
        f_event(hop)
    for b in range(batch):
        x_end(b)
    store_mixed(steps - 2).wait()
    store_mixed(steps - 1).wait()
    w_end()


def gather(queries, keys_in, values_in, out_weight, count):
    batch, tokens, heads, size = keys_in.shape
    depth, lanes = lax.axis_size("dp"), lax.axis_size("sp")
    places = lanes // 2
    rows, width = out_weight.shape
    held, deep = heads // 2, size + EXTRA
    tile = min(TILE, tokens)
    any_space = pl.BlockSpec(memory_space=pl.ANY)
    dma = pltpu.SemaphoreType.DMA
    f32, bf16 = jnp.float32, jnp.bfloat16
    w_dma = dma((2, depth, 2))
    return pl.pallas_call(
        functools.partial(
            gather_kernel, (depth, lanes), count, tile, batch, tokens, heads, size
        ),
        out_shape=(
            jax.ShapeDtypeStruct((batch * tokens, heads * size), bf16),
            jax.ShapeDtypeStruct((depth * rows, width), bf16),
        ),
        in_specs=[any_space] * 4,
        out_specs=(any_space, any_space),
        scratch_shapes=[
            pltpu.VMEM((SLOTS, tile, heads, size), bf16),
            pltpu.VMEM((SLOTS, tile, heads, size), bf16),
            pltpu.VMEM((SLOTS, tile, heads, size), bf16),
            pltpu.VMEM((2, tile, heads * size), bf16),
            pltpu.VMEM((tile * PITCH, size), f32),
            pltpu.VMEM((tile * PITCH, size), f32),
            pltpu.VMEM((batch, heads, deep, size), f32),
            pltpu.VMEM((batch, held, deep, size), f32),
            pltpu.VMEM((batch, held, deep, size), bf16),
            pltpu.VMEM((batch, places - 1, held // places, deep, size), bf16),
            pltpu.VMEM((batch, heads, deep, size), bf16),
            pltpu.VMEM((heads, 2 * size, 2 * size), bf16),
            pltpu.VMEM((depth, rows, width), bf16),
            dma((2, SLOTS)),
            dma((SLOTS,)),
            dma((2,)),
            dma,
            dma((2, depth)),
            w_dma, w_dma, w_dma, w_dma, w_dma, w_dma, w_dma, w_dma,
            dma((batch,)),
            dma((batch,)),
            dma((batch, places)),
            dma((batch, places)),
            dma((batch, places)),
            dma((batch, places)),
            dma((batch,)),
            dma((batch,)),
        ],
        compiler_params=pltpu.CompilerParams(
            collective_id=0, has_side_effects=True, vmem_limit_bytes=60 * 2**20
        ),
    )(queries, keys_in, values_in, out_weight)


def on_device(queries_in, keys_in, values_in, out_weight):
    batch, tokens = queries_in.shape[:2]
    count = tokens * lax.axis_size("sp")
    mixed, wide = gather(queries_in, keys_in, values_in, out_weight, count)
    out = jnp.dot(mixed, wide, preferred_element_type=jnp.float32).astype(jnp.bfloat16)
    return out.reshape(batch, tokens, wide.shape[1])


def solution(mesh):
    placed = (
        P("dp", "sp", None, None),
        P("dp", "sp", None, None),
        P("dp", "sp", None, None),
        P("dp", None),
    )
    return jax.shard_map(
        on_device, mesh=mesh, in_specs=placed, out_specs=P("dp", "sp", None), check_vma=False
    )
```

```python
import functools

import jax
import jax.numpy as jnp
from jax import lax
from jax.experimental import pallas as pl
from jax.experimental.pallas import tpu as pltpu
from jax.sharding import PartitionSpec as P

MESH = pl.DeviceIdType.MESH
SLOTS = 3
TILE = 256
SUBLANES = 8
PITCH = 24
EXTRA = 16
CUTS = 2
GROUP = 32
REGIONS = 8
T_FOLD, T_Z = 4.0, 4.2
D_FOLD, D_PREPARE, D_TABLE, D_READ, D_PROJECT = 1.2, 0.75, 1.0, 0.8, 1.3
D_Z, D_N, D_C, D_R, D_G = 2.81, 4.5, 2.0, 5.6, 5.6


def feature_map(values):
    wide = values.astype(jnp.float32)
    return wide * wide + 0.1


def split_mass(mass):
    high = mass.astype(jnp.bfloat16).astype(jnp.float32)
    row = lax.broadcasted_iota(jnp.int32, mass.shape, mass.ndim - 2)
    return jnp.where(row % 2 == 0, high, mass - high).astype(jnp.bfloat16)


def gather_kernel(
    groups, count, tile, batch, tokens, heads, size,
    q_ref, k_ref, v_ref, w_ref, mixed, w_all, acc,
    k_buf, v_buf, q_buf, regions, rel_k, total, core_in, out_buf, in_buf,
    final, table, load_sem, q_sem, own_sem,
    z_send, z_recv, n_send, n_recv, p_send, p_recv, m_send, m_recv,
    c_send, c_recv, r_send, r_recv, g_send, g_recv, f_send, f_recv,
):
    f32, bf16 = jnp.float32, jnp.bfloat16
    depth, lanes = groups
    places = lanes // 2
    levels = places.bit_length() - 1
    d, s = lax.axis_index("dp"), lax.axis_index("sp")
    core, place = s % 2, s // 2
    rows, width = w_ref.shape
    part, half_width = rows // 4, width // 2
    cut = part // CUTS
    pieces = [(r, side) for r in range(CUTS) for side in range(2)]
    per_batch = tokens // tile
    steps = batch * per_batch
    held = heads // 2
    piece = held // places
    root = count**0.5

    def flip(value, bit):
        return value + (1 << bit) - 2 * (1 << bit) * ((value // (1 << bit)) % 2)

    def peer_place(k):
        other = place
        for bit in range(levels):
            if k >> bit & 1:
                other = flip(other, bit)
        return other

    partner = {"sp": flip(s, 0)}
    peers = [{"sp": 2 * peer_place(k) + core} for k in range(1, places)]
    sides = [{"sp": flip(s, 1)}, {"sp": flip(s, levels)}]
    parity = place % 2
    if levels > 1:
        parity = (parity + (place // (1 << (levels - 1))) % 2) % 2
    quarter, across = parity * 2 + core, (1 - parity) * 2 + core

    barrier = pltpu.get_barrier_semaphore()
    for device in [partner] + peers + [{"dp": (d + k) % depth} for k in (1, depth - 1)]:
        pl.semaphore_signal(barrier, inc=1, device_id=device, device_id_type=MESH)

    def load(i):
        b, t, slot = i // per_batch, i % per_batch, i % SLOTS
        at = pl.ds(t * tile, tile)
        return (
            pltpu.make_async_copy(k_ref.at[b, at], k_buf.at[slot], load_sem.at[0, slot]),
            pltpu.make_async_copy(v_ref.at[b, at], v_buf.at[slot], load_sem.at[1, slot]),
        )

    def load_q(i):
        b, t, slot = i // per_batch, i % per_batch, i % SLOTS
        return pltpu.make_async_copy(
            q_ref.at[b, pl.ds(t * tile, tile)], q_buf.at[slot], q_sem.at[slot]
        )

    for i in range(min(SLOTS - 1, steps)):
        for copy in load(i):
            copy.start()
    own = pltpu.make_async_copy(w_ref, w_all.at[d], own_sem)
    own.start()
    total[...] = jnp.zeros_like(total)
    table[...] = jnp.zeros_like(table)
    pl.semaphore_wait(barrier, places + 2)

    def origin(way, hop):
        return d - hop if way == 0 else d + hop

    def inside(place_on_dp):
        return jnp.logical_and(place_on_dp >= 0, place_on_dp < depth)

    def sends(way, hop):
        return jnp.logical_and(inside(origin(way, hop - 1)), inside(origin(way, -1)))

    def block(from_dp, index, c):
        r, side = pieces[c]
        return w_all.at[
            from_dp, pl.ds(index * part + r * cut, cut), pl.ds(side * half_width, half_width)
        ]

    def z_copy(way, hop, c):
        target = block(origin(way, hop - 1), quarter, c)
        source = target
        if hop == 1:
            r, side = pieces[c]
            source = w_ref.at[
                pl.ds(quarter * part + r * cut, cut), pl.ds(side * half_width, half_width)
            ]
        return pltpu.make_async_remote_copy(
            src_ref=source, dst_ref=target,
            send_sem=z_send.at[way, hop, c], recv_sem=z_recv.at[way, hop, c],
            device_id={"dp": (d + (1 if way == 0 else depth - 1)) % depth},
            device_id_type=MESH,
        )

    def z_arrival(way, hop, c):
        target = block(origin(way, hop), quarter, c)
        return pltpu.make_async_remote_copy(
            src_ref=target, dst_ref=target,
            send_sem=z_send.at[way, hop, c], recv_sem=z_recv.at[way, hop, c],
            device_id={"dp": (d + 1) % depth}, device_id_type=MESH,
        )

    def spread(way, hop, c, index, send, recv, device):
        target = block(origin(way, hop), index, c)
        return pltpu.make_async_remote_copy(
            src_ref=target, dst_ref=target,
            send_sem=send.at[way, hop, c], recv_sem=recv.at[way, hop, c],
            device_id=device, device_id_type=MESH,
        )

    def n_copy(way, hop, c):
        return spread(way, hop, c, quarter, n_send, n_recv, sides[pieces[c][1]])

    def p_copy(way, hop, c):
        return spread(way, hop, c, quarter, p_send, p_recv, partner)

    def m_copy(way, hop, c):
        return spread(way, hop, c, across, m_send, m_recv, partner)

    def each_way(hop, act):
        for way in range(2):
            pl.when(inside(origin(way, hop)))(functools.partial(act, way))

    done = set()

    def once(*key):
        fresh = key[1] < depth and key not in done
        done.add(key)
        return fresh

    def z_event(hop, c):
        if not once("z", hop, c):
            return
        each_way(hop, lambda way: z_arrival(way, hop, c).wait_recv())
        if hop + 1 < depth:
            for way in range(2):
                pl.when(sends(way, hop + 1))(lambda way=way: z_copy(way, hop + 1, c).start())

        def forward(way):
            n_copy(way, hop, c).start()
            p_copy(way, hop, c).start()

        each_way(hop, forward)

    def n_event(hop, c):
        if not once("n", hop, c):
            return

        def act(way):
            n_copy(way, hop, c).wait_recv()
            m_copy(way, hop, c).start()

        each_way(hop, act)

    def f_event(hop):
        if not once("f", hop):
            return
        for c in range(len(pieces)):
            z_event(hop, c)
        for c in range(len(pieces)):
            n_event(hop, c)

        def act(way):
            for c in range(len(pieces)):
                p_copy(way, hop, c).wait_recv()
                m_copy(way, hop, c).wait_recv()

        each_way(hop, act)

    def w_end():
        for hop in range(1, depth):
            f_event(hop)
        for hop in range(1, depth):
            for way in range(2):
                for c in range(len(pieces)):
                    pl.when(sends(way, hop))(
                        lambda way=way, hop=hop, c=c: z_copy(way, hop, c).wait_send()
                    )

            def act(way, hop=hop):
                for c in range(len(pieces)):
                    for make in (n_copy, p_copy, m_copy):
                        make(way, hop, c).wait_send()

            each_way(hop, act)

    for c in range(len(pieces)):
        for way in range(2):
            pl.when(sends(way, 1))(lambda way=way, c=c: z_copy(way, 1, c).start())

    def c_copy(b):
        return pltpu.make_async_remote_copy(
            src_ref=total.at[b, pl.ds((1 - core) * held, held)], dst_ref=core_in.at[b],
            send_sem=c_send.at[b], recv_sem=c_recv.at[b],
            device_id=partner, device_id_type=MESH,
        )

    def r_copy(b, k):
        return pltpu.make_async_remote_copy(
            src_ref=out_buf.at[b, pl.ds(peer_place(k) * piece, piece)],
            dst_ref=in_buf.at[b, k - 1],
            send_sem=r_send.at[b, k], recv_sem=r_recv.at[b, k],
            device_id=peers[k - 1], device_id_type=MESH,
        )

    def g_copy(b, k):
        at = final.at[b, pl.ds(core * held + place * piece, piece)]
        return pltpu.make_async_remote_copy(
            src_ref=at, dst_ref=at, send_sem=g_send.at[b, k], recv_sem=g_recv.at[b, k],
            device_id=peers[k - 1], device_id_type=MESH,
        )

    def f_copy(b):
        at = final.at[b, pl.ds(core * held, held)]
        return pltpu.make_async_remote_copy(
            src_ref=at, dst_ref=at, send_sem=f_send.at[b], recv_sem=f_recv.at[b],
            device_id=partner, device_id_type=MESH,
        )

    def x_add(b):
        c_copy(b).wait()
        mine = pl.ds(core * held, held)
        summed = total[b, mine] + core_in[b]
        total[b, mine] = summed
        out_buf[b, :, :size] = summed[:, :size].astype(bf16)
        out_buf[b, :, size:] = split_mass(summed[:, size:])
        for k in range(1, places):
            r_copy(b, k).start()

    def x_sum(b):
        mine = pl.ds(core * held + place * piece, piece)
        state, mass = total[b, mine, :size], total[b, mine, size:]
        for k in range(1, places):
            r_copy(b, k).wait_recv()
            state += in_buf[b, k - 1, :, :size].astype(f32)
            pair = in_buf[b, k - 1, :, size:].astype(f32)
            mass += pair[:, :1] + pair[:, 1:2]
        final[b, mine, :size] = (state / count).astype(bf16)
        final[b, mine, size:] = split_mass(mass / count / root)
        for k in range(1, places):
            g_copy(b, k).start()

    def x_share(b):
        for k in range(1, places):
            g_copy(b, k).wait_recv()
        f_copy(b).start()

    def x_table(b):
        f_copy(b).wait_recv()
        for h in range(heads):
            pair = final[b, h, size:].astype(f32)
            table[h, :size, :size] = final[b, h, :size]
            table[h, size:, :size] = jnp.broadcast_to(pair[:1], (size, size)).astype(bf16)
            table[h, size:, size:] = jnp.broadcast_to(pair[1:2], (size, size)).astype(bf16)

    def x_end(b):
        for k in range(1, places):
            r_copy(b, k).wait_send()
            g_copy(b, k).wait_send()
        f_copy(b).wait_send()

    groups_of = tile // GROUP

    def regroup(g, values, store):
        region = regions[g % REGIONS]
        for part_of in range(heads // SUBLANES):
            start = part_of * SUBLANES
            region.at[part_of].reshape(GROUP, SUBLANES, size)[...] = values[
                :, start : start + SUBLANES
            ]
        for h in range(heads):
            line = pl.ds(h % SUBLANES, GROUP, stride=SUBLANES)
            store(h, region[h // SUBLANES, line, :].astype(bf16))

    ones = jnp.ones((EXTRA, tile), bf16)

    def fold(i):
        slot, b = i % SLOTS, i // per_batch
        rel_k.reshape(tile, PITCH, size)[:, :heads, :] = feature_map(k_buf[slot])
        v_heads = pltpu.einshape("thd->htd", v_buf[slot])
        for h in range(heads):
            left = jnp.concatenate([jnp.transpose(v_heads[h]), ones], axis=0)
            right = rel_k[pl.ds(h, tile, stride=PITCH), :].astype(bf16)
            total[b, h] += jnp.dot(left, right, preferred_element_type=f32)

    def spot(i, h):
        block_of, column = divmod(h * size, rows)
        return block_of, pl.ds(i * tile, tile), pl.ds(column, size)

    def prepare(i):
        for g in range(groups_of):
            def put(h, x, g=g):
                block_of, column = divmod(h * size, rows)
                at = pl.ds(i * tile + g * GROUP, GROUP)
                mixed[block_of, at, pl.ds(column, size)] = x

            regroup(g, feature_map(q_buf[i % SLOTS, pl.ds(g * GROUP, GROUP)]), put)

    def read(i):
        for h in range(heads):
            feature = mixed[spot(i, h)]
            both = lax.dot_general(
                jnp.concatenate([feature, feature], axis=1), table[h],
                (((1,), (1,)), ((), ())), preferred_element_type=f32,
            )
            top = both[:, :size] / (both[:, size:] + 0.001 / root)
            mixed[spot(i, h)] = top.astype(bf16)

    broad = min(2 * tile, tokens)

    def project(i, j):
        at, source = pl.ds(i * broad, broad), nearest(d, depth, j)
        product = jnp.dot(mixed[source, at], w_all[source], preferred_element_type=f32)
        acc[at, :] = product if j == 0 else acc[at, :] + product

    def at_step(i, events):
        for moment, items in events.items():
            if not items:
                continue

            def run(items=items):
                for item in items:
                    item()

            pl.when(i == moment)(run)

    def make(function, *args):
        return functools.partial(function, *args)

    plan, clock = [], [T_FOLD]

    def due():
        now = []
        while plan and plan[0][0] <= clock[0]:
            now.append(plan.pop(0)[1])
        return now

    def run_due():
        for event in due():
            event()

    def loop(start, stop, body, length, extra=None):
        events = {}
        for i in range(start, stop):
            events[i] = (extra or {}).get(i, []) + due()
            clock[0] += length

        def one(i, carry):
            at_step(i, events)
            body(i)
            return carry

        lax.fori_loop(start, stop, one, 0)

    def fold_step(i):
        @pl.when(i + SLOTS - 1 < steps)
        def _():
            for copy in load(i + SLOTS - 1):
                copy.start()

        @pl.when(i + SLOTS - 1 >= steps)
        def _():
            load_q(i + SLOTS - 1 - steps).start()

        for copy in load(i):
            copy.wait()
        fold(i)

    def prepare_step(i):
        @pl.when(i + SLOTS - 1 < steps)
        def _():
            load_q(i + SLOTS - 1).start()

        load_q(i).wait()
        prepare(i)

    half = per_batch
    t_half = T_FOLD + half * D_FOLD
    t_full = T_FOLD + steps * D_FOLD
    for hop in range(1, depth):
        for c in range(len(pieces)):
            arrival = T_Z + D_Z * (len(pieces) * (hop - 1) + c + 1)
            plan.append((arrival, make(z_event, hop, c)))
            plan.append((arrival + D_N, make(n_event, hop, c)))
    plan.append((t_half + D_C, make(x_add, 0)))
    plan.append((t_half + D_C + D_R, make(x_sum, 0)))
    plan.append((t_half + D_C + D_R + D_G, make(x_share, 0)))
    plan.append((t_full + D_C, make(x_add, 1)))
    plan.append((t_full + D_C + D_R, make(x_sum, 1)))
    plan.append((t_full + D_C + D_R + D_G, make(x_share, 1)))
    plan.sort(key=lambda item: item[0])

    def require(name, b):
        for index, item in enumerate(plan):
            if item[1].func is name and item[1].args == (b,):
                for _ in range(index + 1):
                    plan.pop(0)[1]()
                clock[0] = max(clock[0], item[0])
                return

    loop(0, steps, fold_step, D_FOLD, {half: [lambda: c_copy(0).start()]})
    c_copy(1).start()
    loop(0, steps, prepare_step, D_PREPARE)
    own.wait()
    require(x_share, 0)
    run_due()
    x_table(0)
    clock[0] += D_TABLE
    loop(0, half, read, D_READ)
    mid = half * tile // broad
    end = 2 * mid
    loop(0, mid, lambda i: project(i, 0), D_PROJECT)
    require(x_share, 1)
    run_due()
    x_table(1)
    clock[0] += D_TABLE
    loop(half, steps, read, D_READ)
    loop(mid, end, lambda i: project(i, 0), D_PROJECT)
    for j in range(1, depth - 1):
        f_event(j)
        loop(0, end, lambda i, j=j: project(i, j), D_PROJECT)
    for b in range(batch):
        x_end(b)
    w_end()


def nearest(d, depth, j):
    both = 2 * jnp.minimum(d, depth - 1 - d)
    around = d - (j + 1) // 2 if j % 2 else d + j // 2
    return jnp.where(j <= both, around, jnp.where(d < depth - 1 - d, j, depth - 1 - j))


def close_kernel(depth, tile, acc, mixed, w_all, out_ref, stage, sem):
    source = nearest(lax.axis_index("dp"), depth, depth - 1)
    steps = acc.shape[0] // tile

    def store(i):
        return pltpu.make_async_copy(
            stage.at[i % 2], out_ref.at[pl.ds(i * tile, tile)], sem.at[i % 2]
        )

    def step(i, carry):
        at = pl.ds(i * tile, tile)
        pl.when(i > 1)(lambda: store(i - 2).wait())
        product = jnp.dot(mixed[source, at], w_all[source], preferred_element_type=jnp.float32)
        stage[i % 2] = (acc[at, :] + product).astype(jnp.bfloat16)
        store(i).start()
        return carry

    lax.fori_loop(0, steps, step, 0)
    for i in range(max(steps - 2, 0), steps):
        store(i).wait()


def close(acc, mixed, w_all, tile):
    vmem = pl.BlockSpec(memory_space=pltpu.VMEM)
    total, width = acc.shape
    return pl.pallas_call(
        functools.partial(close_kernel, w_all.shape[0], tile),
        out_shape=jax.ShapeDtypeStruct((total, width), jnp.bfloat16),
        in_specs=[vmem] * 3,
        out_specs=pl.BlockSpec(memory_space=pl.ANY),
        scratch_shapes=[
            pltpu.VMEM((2, tile, width), jnp.bfloat16),
            pltpu.SemaphoreType.DMA((2,)),
        ],
        compiler_params=pltpu.CompilerParams(vmem_limit_bytes=8 * 2**20),
    )(acc, mixed, w_all)


def gather(queries, keys_in, values_in, out_weight, count):
    batch, tokens, heads, size = keys_in.shape
    depth, lanes = lax.axis_size("dp"), lax.axis_size("sp")
    places = lanes // 2
    rows, width = out_weight.shape
    held, deep = heads // 2, size + EXTRA
    tile = min(TILE, tokens)
    any_space = pl.BlockSpec(memory_space=pl.ANY)
    dma = pltpu.SemaphoreType.DMA
    f32, bf16 = jnp.float32, jnp.bfloat16
    w_dma = dma((2, depth, 2 * CUTS))
    vmem = pl.BlockSpec(memory_space=pltpu.VMEM)
    return pl.pallas_call(
        functools.partial(
            gather_kernel, (depth, lanes), count, tile, batch, tokens, heads, size
        ),
        out_shape=(
            pltpu.VMEM((depth, batch * tokens, rows), bf16),
            pltpu.VMEM((depth, rows, width), bf16),
            pltpu.VMEM((batch * tokens, width), f32),
        ),
        in_specs=[any_space] * 4,
        out_specs=(vmem, vmem, vmem),
        scratch_shapes=[
            pltpu.VMEM((SLOTS, tile, heads, size), bf16),
            pltpu.VMEM((SLOTS, tile, heads, size), bf16),
            pltpu.VMEM((SLOTS, tile, heads, size), bf16),
            [pltpu.VMEM((heads // SUBLANES, GROUP * SUBLANES, size), f32)] * REGIONS,
            pltpu.VMEM((tile * PITCH, size), f32),
            pltpu.VMEM((batch, heads, deep, size), f32),
            pltpu.VMEM((batch, held, deep, size), f32),
            pltpu.VMEM((batch, held, deep, size), bf16),
            pltpu.VMEM((batch, places - 1, held // places, deep, size), bf16),
            pltpu.VMEM((batch, heads, deep, size), bf16),
            pltpu.VMEM((heads, 2 * size, 2 * size), bf16),
            dma((2, SLOTS)),
            dma((SLOTS,)),
            dma,
            w_dma, w_dma, w_dma, w_dma, w_dma, w_dma, w_dma, w_dma,
            dma((batch,)),
            dma((batch,)),
            dma((batch, places)),
            dma((batch, places)),
            dma((batch, places)),
            dma((batch, places)),
            dma((batch,)),
            dma((batch,)),
        ],
        compiler_params=pltpu.CompilerParams(
            collective_id=0, has_side_effects=True, vmem_limit_bytes=26 * 2**20
        ),
    )(queries, keys_in, values_in, out_weight)


def on_device(queries_in, keys_in, values_in, out_weight):
    batch, tokens = queries_in.shape[:2]
    count = tokens * lax.axis_size("sp")
    mixed, w_all, acc = gather(queries_in, keys_in, values_in, out_weight, count)
    out = close(acc, mixed, w_all, min(2 * TILE, tokens))
    return out.reshape(batch, tokens, out_weight.shape[1])


def solution(mesh):
    placed = (
        P("dp", "sp", None, None),
        P("dp", "sp", None, None),
        P("dp", "sp", None, None),
        P("dp", None),
    )
    return jax.shard_map(
        on_device, mesh=mesh, in_specs=placed, out_specs=P("dp", "sp", None), check_vma=False
    )
```

```python
import functools

import jax
import jax.numpy as jnp
from jax import lax
from jax.experimental import pallas as pl
from jax.experimental.pallas import tpu as pltpu
from jax.sharding import PartitionSpec as P

MESH = pl.DeviceIdType.MESH
SLOTS = 3
TILE = 256
SUBLANES = 8
PITCH = 24
EXTRA = 16
CUTS = 2
GROUP = 32
REGIONS = 8
T_FOLD, T_Z = 4.0, 6.0
D_FOLD, D_PREPARE, D_TABLE, D_READ, D_PROJECT = 1.2, 0.75, 1.0, 0.8, 1.3
D_Z, D_N, D_C, D_R, D_G = 2.81, 4.5, 1.8, 4.6, 4.6
HOLD = 0.0


def feature_map(values):
    wide = values.astype(jnp.float32)
    return wide * wide + 0.1


def split_mass(mass):
    high = mass.astype(jnp.bfloat16).astype(jnp.float32)
    row = lax.broadcasted_iota(jnp.int32, mass.shape, mass.ndim - 2)
    return jnp.where(row % 2 == 0, high, mass - high).astype(jnp.bfloat16)


def gather_kernel(
    groups, count, tile, batch, tokens, heads, size,
    q_ref, k_ref, v_ref, w_ref, mixed, w_all, acc,
    k_buf, v_buf, q_buf, regions, rel_k, total, core_in, out_buf, in_buf,
    final, table, load_sem, q_sem, own_sem,
    z_send, z_recv, n_send, n_recv, p_send, p_recv, m_send, m_recv,
    c_send, c_recv, r_send, r_recv, g_send, g_recv, f_send, f_recv,
):
    f32, bf16 = jnp.float32, jnp.bfloat16
    depth, lanes = groups
    places = lanes // 2
    levels = places.bit_length() - 1
    d, s = lax.axis_index("dp"), lax.axis_index("sp")
    core, place = s % 2, s // 2
    rows, width = w_ref.shape
    part, half_width = rows // 4, width // 2
    cut = part // CUTS
    pieces = [(r, side) for r in range(CUTS) for side in range(2)]
    per_batch = tokens // tile
    steps = batch * per_batch
    held = heads // 2
    piece = held // places
    root = count**0.5

    def flip(value, bit):
        return value + (1 << bit) - 2 * (1 << bit) * ((value // (1 << bit)) % 2)

    def peer_place(k):
        other = place
        for bit in range(levels):
            if k >> bit & 1:
                other = flip(other, bit)
        return other

    partner = {"sp": flip(s, 0)}
    peers = [{"sp": 2 * peer_place(k) + core} for k in range(1, places)]
    sides = [{"sp": flip(s, 1)}, {"sp": flip(s, levels)}]
    parity = place % 2
    if levels > 1:
        parity = (parity + (place // (1 << (levels - 1))) % 2) % 2
    quarter, across = parity * 2 + core, (1 - parity) * 2 + core

    barrier = pltpu.get_barrier_semaphore()
    for device in [partner] + peers + [{"dp": (d + k) % depth} for k in (1, depth - 1)]:
        pl.semaphore_signal(barrier, inc=1, device_id=device, device_id_type=MESH)

    def load(i):
        b, t, slot = i // per_batch, i % per_batch, i % SLOTS
        at = pl.ds(t * tile, tile)
        return (
            pltpu.make_async_copy(k_ref.at[b, at], k_buf.at[slot], load_sem.at[0, slot]),
            pltpu.make_async_copy(v_ref.at[b, at], v_buf.at[slot], load_sem.at[1, slot]),
        )

    def load_q(i):
        b, t, slot = i // per_batch, i % per_batch, i % SLOTS
        return pltpu.make_async_copy(
            q_ref.at[b, pl.ds(t * tile, tile)], q_buf.at[slot], q_sem.at[slot]
        )

    for i in range(min(SLOTS - 1, steps)):
        for copy in load(i):
            copy.start()
    own = pltpu.make_async_copy(w_ref, w_all.at[d], own_sem)
    own.start()
    total[...] = jnp.zeros_like(total)
    table[...] = jnp.zeros_like(table)
    pl.semaphore_wait(barrier, places + 2)

    def origin(way, hop):
        return d - hop if way == 0 else d + hop

    def inside(place_on_dp):
        return jnp.logical_and(place_on_dp >= 0, place_on_dp < depth)

    def sends(way, hop):
        return jnp.logical_and(inside(origin(way, hop - 1)), inside(origin(way, -1)))

    def block(from_dp, index, c):
        r, side = pieces[c]
        return w_all.at[
            from_dp, pl.ds(index * part + r * cut, cut), pl.ds(side * half_width, half_width)
        ]

    def z_copy(way, hop, c):
        target = block(origin(way, hop - 1), quarter, c)
        source = target
        if hop == 1:
            r, side = pieces[c]
            source = w_ref.at[
                pl.ds(quarter * part + r * cut, cut), pl.ds(side * half_width, half_width)
            ]
        return pltpu.make_async_remote_copy(
            src_ref=source, dst_ref=target,
            send_sem=z_send.at[way, hop, c], recv_sem=z_recv.at[way, hop, c],
            device_id={"dp": (d + (1 if way == 0 else depth - 1)) % depth},
            device_id_type=MESH,
        )

    def z_arrival(way, hop, c):
        target = block(origin(way, hop), quarter, c)
        return pltpu.make_async_remote_copy(
            src_ref=target, dst_ref=target,
            send_sem=z_send.at[way, hop, c], recv_sem=z_recv.at[way, hop, c],
            device_id={"dp": (d + 1) % depth}, device_id_type=MESH,
        )

    def spread(way, hop, c, index, send, recv, device):
        target = block(origin(way, hop), index, c)
        return pltpu.make_async_remote_copy(
            src_ref=target, dst_ref=target,
            send_sem=send.at[way, hop, c], recv_sem=recv.at[way, hop, c],
            device_id=device, device_id_type=MESH,
        )

    def n_copy(way, hop, c):
        return spread(way, hop, c, quarter, n_send, n_recv, sides[pieces[c][1]])

    def p_copy(way, hop, c):
        return spread(way, hop, c, quarter, p_send, p_recv, partner)

    def m_copy(way, hop, c):
        return spread(way, hop, c, across, m_send, m_recv, partner)

    def each_way(hop, act):
        for way in range(2):
            pl.when(inside(origin(way, hop)))(functools.partial(act, way))

    done = set()

    def once(*key):
        fresh = key[1] < depth and key not in done
        done.add(key)
        return fresh

    def z_event(hop, c):
        if not once("z", hop, c):
            return
        each_way(hop, lambda way: z_arrival(way, hop, c).wait_recv())
        if hop + 1 < depth:
            for way in range(2):
                pl.when(sends(way, hop + 1))(lambda way=way: z_copy(way, hop + 1, c).start())

    def s_event(hop, c):
        if not once("s", hop, c):
            return

        def act(way):
            n_copy(way, hop, c).start()
            p_copy(way, hop, c).start()

        each_way(hop, act)

    def n_event(hop, c):
        if not once("n", hop, c):
            return

        def act(way):
            n_copy(way, hop, c).wait_recv()
            m_copy(way, hop, c).start()

        each_way(hop, act)

    def f_event(hop):
        if not once("f", hop):
            return
        for event in (z_event, s_event, n_event):
            for c in range(len(pieces)):
                event(hop, c)

        def act(way):
            for c in range(len(pieces)):
                p_copy(way, hop, c).wait_recv()
                m_copy(way, hop, c).wait_recv()

        each_way(hop, act)

    def w_end():
        for hop in range(1, depth):
            f_event(hop)
        for hop in range(1, depth):
            for way in range(2):
                for c in range(len(pieces)):
                    pl.when(sends(way, hop))(
                        lambda way=way, hop=hop, c=c: z_copy(way, hop, c).wait_send()
                    )

            def act(way, hop=hop):
                for c in range(len(pieces)):
                    for make in (n_copy, p_copy, m_copy):
                        make(way, hop, c).wait_send()

            each_way(hop, act)

    for c in range(len(pieces)):
        for way in range(2):
            pl.when(sends(way, 1))(lambda way=way, c=c: z_copy(way, 1, c).start())

    def c_copy(b):
        return pltpu.make_async_remote_copy(
            src_ref=total.at[b, pl.ds((1 - core) * held, held)], dst_ref=core_in.at[b],
            send_sem=c_send.at[b], recv_sem=c_recv.at[b],
            device_id=partner, device_id_type=MESH,
        )

    def r_copy(b, k):
        return pltpu.make_async_remote_copy(
            src_ref=out_buf.at[b, pl.ds(peer_place(k) * piece, piece)],
            dst_ref=in_buf.at[b, k - 1],
            send_sem=r_send.at[b, k], recv_sem=r_recv.at[b, k],
            device_id=peers[k - 1], device_id_type=MESH,
        )

    def g_copy(b, k):
        at = final.at[b, pl.ds(core * held + place * piece, piece)]
        return pltpu.make_async_remote_copy(
            src_ref=at, dst_ref=at, send_sem=g_send.at[b, k], recv_sem=g_recv.at[b, k],
            device_id=peers[k - 1], device_id_type=MESH,
        )

    def f_copy(b):
        at = final.at[b, pl.ds(core * held, held)]
        return pltpu.make_async_remote_copy(
            src_ref=at, dst_ref=at, send_sem=f_send.at[b], recv_sem=f_recv.at[b],
            device_id=partner, device_id_type=MESH,
        )

    def x_add(b):
        c_copy(b).wait()
        mine = pl.ds(core * held, held)
        summed = total[b, mine] + core_in[b]
        total[b, mine] = summed
        out_buf[b, :, :size] = summed[:, :size].astype(bf16)
        out_buf[b, :, size:] = split_mass(summed[:, size:])
        for k in range(1, places):
            r_copy(b, k).start()

    def x_sum(b):
        mine = pl.ds(core * held + place * piece, piece)
        state, mass = total[b, mine, :size], total[b, mine, size:]
        for k in range(1, places):
            r_copy(b, k).wait_recv()
            state += in_buf[b, k - 1, :, :size].astype(f32)
            pair = in_buf[b, k - 1, :, size:].astype(f32)
            mass += pair[:, :1] + pair[:, 1:2]
        final[b, mine, :size] = (state / count).astype(bf16)
        final[b, mine, size:] = split_mass(mass / count / root)
        for k in range(1, places):
            g_copy(b, k).start()

    def x_share(b):
        for k in range(1, places):
            g_copy(b, k).wait_recv()
        f_copy(b).start()

    def x_table(b):
        f_copy(b).wait_recv()
        for h in range(heads):
            pair = final[b, h, size:].astype(f32)
            table[h, :size, :size] = final[b, h, :size]
            table[h, size:, :size] = jnp.broadcast_to(pair[:1], (size, size)).astype(bf16)
            table[h, size:, size:] = jnp.broadcast_to(pair[1:2], (size, size)).astype(bf16)

    def x_end(b):
        for k in range(1, places):
            r_copy(b, k).wait_send()
            g_copy(b, k).wait_send()
        f_copy(b).wait_send()

    groups_of = tile // GROUP

    def regroup(g, values, store):
        region = regions[g % REGIONS]
        for part_of in range(heads // SUBLANES):
            start = part_of * SUBLANES
            region.at[part_of].reshape(GROUP, SUBLANES, size)[...] = values[
                :, start : start + SUBLANES
            ]
        for h in range(heads):
            line = pl.ds(h % SUBLANES, GROUP, stride=SUBLANES)
            store(h, region[h // SUBLANES, line, :].astype(bf16))

    ones = jnp.ones((EXTRA, tile), bf16)

    def fold(i):
        slot, b = i % SLOTS, i // per_batch
        rel_k.reshape(tile, PITCH, size)[:, :heads, :] = feature_map(k_buf[slot])
        v_heads = pltpu.einshape("thd->htd", v_buf[slot])
        for h in range(heads):
            left = jnp.concatenate([jnp.transpose(v_heads[h]), ones], axis=0)
            right = rel_k[pl.ds(h, tile, stride=PITCH), :].astype(bf16)
            total[b, h] += jnp.dot(left, right, preferred_element_type=f32)

    def spot(i, h):
        block_of, column = divmod(h * size, rows)
        return block_of, pl.ds(i * tile, tile), pl.ds(column, size)

    def prepare(i):
        for g in range(groups_of):
            def put(h, x, g=g):
                block_of, column = divmod(h * size, rows)
                at = pl.ds(i * tile + g * GROUP, GROUP)
                mixed[block_of, at, pl.ds(column, size)] = x

            regroup(g, feature_map(q_buf[i % SLOTS, pl.ds(g * GROUP, GROUP)]), put)

    def read(i):
        for h in range(heads):
            feature = mixed[spot(i, h)]
            both = lax.dot_general(
                jnp.concatenate([feature, feature], axis=1), table[h],
                (((1,), (1,)), ((), ())), preferred_element_type=f32,
            )
            top = both[:, :size] / (both[:, size:] + 0.001 / root)
            mixed[spot(i, h)] = top.astype(bf16)

    broad = min(2 * tile, tokens)

    def project(i, j):
        at, source = pl.ds(i * broad, broad), nearest(d, depth, j)
        product = jnp.dot(mixed[source, at], w_all[source], preferred_element_type=f32)
        acc[at, :] = product if j == 0 else acc[at, :] + product

    def at_step(i, events):
        for moment, items in events.items():
            if not items:
                continue

            def run(items=items):
                for item in items:
                    item()

            pl.when(i == moment)(run)

    def make(function, *args):
        return functools.partial(function, *args)

    plan, clock = [], [T_FOLD]

    def due():
        now = []
        while plan and plan[0][0] <= clock[0]:
            now.append(plan.pop(0)[1])
        return now

    def run_due():
        for event in due():
            event()

    def loop(start, stop, body, length, extra=None):
        events = {}
        for i in range(start, stop):
            events[i] = (extra or {}).get(i, []) + due()
            clock[0] += length

        def one(i, carry):
            at_step(i, events)
            body(i)
            return carry

        lax.fori_loop(start, stop, one, 0)

    def fold_step(i):
        @pl.when(i + SLOTS - 1 < steps)
        def _():
            for copy in load(i + SLOTS - 1):
                copy.start()

        @pl.when(i + SLOTS - 1 >= steps)
        def _():
            load_q(i + SLOTS - 1 - steps).start()

        for copy in load(i):
            copy.wait()
        fold(i)

    def prepare_step(i):
        @pl.when(i + SLOTS - 1 < steps)
        def _():
            load_q(i + SLOTS - 1).start()

        load_q(i).wait()
        prepare(i)

    half = per_batch
    t_half = T_FOLD + half * D_FOLD
    t_full = T_FOLD + steps * D_FOLD
    free = [0.0, 0.0]
    for hop in range(1, depth):
        for c in range(len(pieces)):
            arrival = T_Z + D_Z * (len(pieces) * (hop - 1) + c + 1)
            ready, side = max(arrival, HOLD), pieces[c][1]
            free[side] = max(free[side], ready) + D_Z * (2 if hop == 1 else 1)
            plan.append((arrival, make(z_event, hop, c)))
            plan.append((ready, make(s_event, hop, c)))
            plan.append((free[side] + D_N, make(n_event, hop, c)))
    plan.append((t_half + D_C, make(x_add, 0)))
    plan.append((t_half + D_C + D_R, make(x_sum, 0)))
    plan.append((t_half + D_C + D_R + D_G, make(x_share, 0)))
    plan.append((t_full + D_C, make(x_add, 1)))
    plan.append((t_full + D_C + D_R, make(x_sum, 1)))
    plan.append((t_full + D_C + D_R + D_G, make(x_share, 1)))
    plan.sort(key=lambda item: item[0])

    def require(name, b):
        for index, item in enumerate(plan):
            if item[1].func is name and item[1].args == (b,):
                for _ in range(index + 1):
                    plan.pop(0)[1]()
                clock[0] = max(clock[0], item[0])
                return

    loop(0, steps, fold_step, D_FOLD, {half: [lambda: c_copy(0).start()]})
    c_copy(1).start()
    loop(0, steps, prepare_step, D_PREPARE)
    own.wait()
    require(x_share, 0)
    run_due()
    x_table(0)
    clock[0] += D_TABLE
    loop(0, half, read, D_READ)
    mid = half * tile // broad
    end = 2 * mid
    loop(0, mid, lambda i: project(i, 0), D_PROJECT)
    require(x_share, 1)
    run_due()
    x_table(1)
    clock[0] += D_TABLE
    loop(half, steps, read, D_READ)
    loop(mid, end, lambda i: project(i, 0), D_PROJECT)
    for j in range(1, depth - 1):
        f_event(j)
        loop(0, end, lambda i, j=j: project(i, j), D_PROJECT)
    for b in range(batch):
        x_end(b)
    w_end()


def nearest(d, depth, j):
    both = 2 * jnp.minimum(d, depth - 1 - d)
    around = d - (j + 1) // 2 if j % 2 else d + j // 2
    return jnp.where(j <= both, around, jnp.where(d < depth - 1 - d, j, depth - 1 - j))


def close_kernel(depth, tile, acc, mixed, w_all, out_ref, stage, sem):
    source = nearest(lax.axis_index("dp"), depth, depth - 1)
    steps = acc.shape[0] // tile

    def store(i):
        return pltpu.make_async_copy(
            stage.at[i % 2], out_ref.at[pl.ds(i * tile, tile)], sem.at[i % 2]
        )

    def step(i, carry):
        at = pl.ds(i * tile, tile)
        pl.when(i > 1)(lambda: store(i - 2).wait())
        product = jnp.dot(mixed[source, at], w_all[source], preferred_element_type=jnp.float32)
        stage[i % 2] = (acc[at, :] + product).astype(jnp.bfloat16)
        store(i).start()
        return carry

    lax.fori_loop(0, steps, step, 0)
    for i in range(max(steps - 2, 0), steps):
        store(i).wait()


def close(acc, mixed, w_all, tile):
    vmem = pl.BlockSpec(memory_space=pltpu.VMEM)
    total, width = acc.shape
    return pl.pallas_call(
        functools.partial(close_kernel, w_all.shape[0], tile),
        out_shape=jax.ShapeDtypeStruct((total, width), jnp.bfloat16),
        in_specs=[vmem] * 3,
        out_specs=pl.BlockSpec(memory_space=pl.ANY),
        scratch_shapes=[
            pltpu.VMEM((2, tile, width), jnp.bfloat16),
            pltpu.SemaphoreType.DMA((2,)),
        ],
        compiler_params=pltpu.CompilerParams(vmem_limit_bytes=8 * 2**20),
    )(acc, mixed, w_all)


def gather(queries, keys_in, values_in, out_weight, count):
    batch, tokens, heads, size = keys_in.shape
    depth, lanes = lax.axis_size("dp"), lax.axis_size("sp")
    places = lanes // 2
    rows, width = out_weight.shape
    held, deep = heads // 2, size + EXTRA
    tile = min(TILE, tokens)
    any_space = pl.BlockSpec(memory_space=pl.ANY)
    dma = pltpu.SemaphoreType.DMA
    f32, bf16 = jnp.float32, jnp.bfloat16
    w_dma = dma((2, depth, 2 * CUTS))
    vmem = pl.BlockSpec(memory_space=pltpu.VMEM)
    return pl.pallas_call(
        functools.partial(
            gather_kernel, (depth, lanes), count, tile, batch, tokens, heads, size
        ),
        out_shape=(
            pltpu.VMEM((depth, batch * tokens, rows), bf16),
            pltpu.VMEM((depth, rows, width), bf16),
            pltpu.VMEM((batch * tokens, width), f32),
        ),
        in_specs=[any_space] * 4,
        out_specs=(vmem, vmem, vmem),
        scratch_shapes=[
            pltpu.VMEM((SLOTS, tile, heads, size), bf16),
            pltpu.VMEM((SLOTS, tile, heads, size), bf16),
            pltpu.VMEM((SLOTS, tile, heads, size), bf16),
            [pltpu.VMEM((heads // SUBLANES, GROUP * SUBLANES, size), f32)] * REGIONS,
            pltpu.VMEM((tile * PITCH, size), f32),
            pltpu.VMEM((batch, heads, deep, size), f32),
            pltpu.VMEM((batch, held, deep, size), f32),
            pltpu.VMEM((batch, held, deep, size), bf16),
            pltpu.VMEM((batch, places - 1, held // places, deep, size), bf16),
            pltpu.VMEM((batch, heads, deep, size), bf16),
            pltpu.VMEM((heads, 2 * size, 2 * size), bf16),
            dma((2, SLOTS)),
            dma((SLOTS,)),
            dma,
            w_dma, w_dma, w_dma, w_dma, w_dma, w_dma, w_dma, w_dma,
            dma((batch,)),
            dma((batch,)),
            dma((batch, places)),
            dma((batch, places)),
            dma((batch, places)),
            dma((batch, places)),
            dma((batch,)),
            dma((batch,)),
        ],
        compiler_params=pltpu.CompilerParams(
            collective_id=0, has_side_effects=True, vmem_limit_bytes=26 * 2**20
        ),
    )(queries, keys_in, values_in, out_weight)


def on_device(queries_in, keys_in, values_in, out_weight):
    batch, tokens = queries_in.shape[:2]
    count = tokens * lax.axis_size("sp")
    mixed, w_all, acc = gather(queries_in, keys_in, values_in, out_weight, count)
    out = close(acc, mixed, w_all, min(2 * TILE, tokens))
    return out.reshape(batch, tokens, out_weight.shape[1])


def solution(mesh):
    placed = (
        P("dp", "sp", None, None),
        P("dp", "sp", None, None),
        P("dp", "sp", None, None),
        P("dp", None),
    )
    return jax.shard_map(
        on_device, mesh=mesh, in_specs=placed, out_specs=P("dp", "sp", None), check_vma=False
    )
```

```python
import functools

import jax
import jax.numpy as jnp
from jax import lax
from jax.experimental import pallas as pl
from jax.experimental.pallas import tpu as pltpu
from jax.sharding import PartitionSpec as P

MESH = pl.DeviceIdType.MESH
SLOTS = 3
TILE = 256
SUBLANES = 8
PITCH = 24
EXTRA = 16
CUTS = 2
GROUP = 32
REGIONS = 8
T_FOLD, T_Z = 4.0, 5.0
D_FOLD, D_PREPARE, D_TABLE, D_READ, D_PROJECT = 1.2, 0.75, 1.0, 0.8, 1.3
D_Z, D_N, D_C, D_R, D_G = 2.81, 4.5, 1.8, 4.6, 4.6
HOLD = 0.0


def feature_map(values):
    wide = values.astype(jnp.float32)
    return wide * wide + 0.1


def split_mass(mass):
    high = mass.astype(jnp.bfloat16).astype(jnp.float32)
    row = lax.broadcasted_iota(jnp.int32, mass.shape, mass.ndim - 2)
    return jnp.where(row % 2 == 0, high, mass - high).astype(jnp.bfloat16)


def gather_kernel(
    groups, count, tile, batch, tokens, heads, size,
    q_ref, k_ref, v_ref, w_ref, mixed, w_all, acc,
    k_buf, v_buf, q_buf, regions, rel_k, total, core_in, out_buf, in_buf,
    final, table, load_sem, q_sem, own_sem,
    z_send, z_recv, n_send, n_recv, p_send, p_recv, m_send, m_recv,
    c_send, c_recv, r_send, r_recv, g_send, g_recv, f_send, f_recv,
):
    f32, bf16 = jnp.float32, jnp.bfloat16
    depth, lanes = groups
    places = lanes // 2
    levels = places.bit_length() - 1
    d, s = lax.axis_index("dp"), lax.axis_index("sp")
    core, place = s % 2, s // 2
    rows, width = w_ref.shape
    part, half_width = rows // 4, width // 2
    cut = part // CUTS
    pieces = [(r, side) for r in range(CUTS) for side in range(2)]
    per_batch = tokens // tile
    steps = batch * per_batch
    held = heads // 2
    piece = held // places
    root = count**0.5

    def flip(value, bit):
        return value + (1 << bit) - 2 * (1 << bit) * ((value // (1 << bit)) % 2)

    def peer_place(k):
        other = place
        for bit in range(levels):
            if k >> bit & 1:
                other = flip(other, bit)
        return other

    partner = {"sp": flip(s, 0)}
    peers = [{"sp": 2 * peer_place(k) + core} for k in range(1, places)]
    sides = [{"sp": flip(s, 1)}, {"sp": flip(s, levels)}]
    parity = place % 2
    if levels > 1:
        parity = (parity + (place // (1 << (levels - 1))) % 2) % 2
    quarter, across = parity * 2 + core, (1 - parity) * 2 + core

    barrier = pltpu.get_barrier_semaphore()
    for device in [partner] + peers + [{"dp": (d + k) % depth} for k in (1, depth - 1)]:
        pl.semaphore_signal(barrier, inc=1, device_id=device, device_id_type=MESH)

    def load(i):
        b, t, slot = i // per_batch, i % per_batch, i % SLOTS
        at = pl.ds(t * tile, tile)
        return (
            pltpu.make_async_copy(k_ref.at[b, at], k_buf.at[slot], load_sem.at[0, slot]),
            pltpu.make_async_copy(v_ref.at[b, at], v_buf.at[slot], load_sem.at[1, slot]),
        )

    def load_q(i):
        b, t, slot = i // per_batch, i % per_batch, i % SLOTS
        return pltpu.make_async_copy(
            q_ref.at[b, pl.ds(t * tile, tile)], q_buf.at[slot], q_sem.at[slot]
        )

    for i in range(min(SLOTS - 1, steps)):
        for copy in load(i):
            copy.start()
    own = pltpu.make_async_copy(w_ref, w_all.at[d], own_sem)
    own.start()
    total[...] = jnp.zeros_like(total)
    table[...] = jnp.zeros_like(table)
    pl.semaphore_wait(barrier, places + 2)

    def origin(way, hop):
        return d - hop if way == 0 else d + hop

    def inside(place_on_dp):
        return jnp.logical_and(place_on_dp >= 0, place_on_dp < depth)

    def sends(way, hop):
        return jnp.logical_and(inside(origin(way, hop - 1)), inside(origin(way, -1)))

    def block(from_dp, index, c):
        r, side = pieces[c]
        return w_all.at[
            from_dp, pl.ds(index * part + r * cut, cut), pl.ds(side * half_width, half_width)
        ]

    def z_copy(way, hop, c):
        target = block(origin(way, hop - 1), quarter, c)
        source = target
        if hop == 1:
            r, side = pieces[c]
            source = w_ref.at[
                pl.ds(quarter * part + r * cut, cut), pl.ds(side * half_width, half_width)
            ]
        return pltpu.make_async_remote_copy(
            src_ref=source, dst_ref=target,
            send_sem=z_send.at[way, hop, c], recv_sem=z_recv.at[way, hop, c],
            device_id={"dp": (d + (1 if way == 0 else depth - 1)) % depth},
            device_id_type=MESH,
        )

    def z_arrival(way, hop, c):
        target = block(origin(way, hop), quarter, c)
        return pltpu.make_async_remote_copy(
            src_ref=target, dst_ref=target,
            send_sem=z_send.at[way, hop, c], recv_sem=z_recv.at[way, hop, c],
            device_id={"dp": (d + 1) % depth}, device_id_type=MESH,
        )

    def spread(way, hop, c, index, send, recv, device):
        target = block(origin(way, hop), index, c)
        return pltpu.make_async_remote_copy(
            src_ref=target, dst_ref=target,
            send_sem=send.at[way, hop, c], recv_sem=recv.at[way, hop, c],
            device_id=device, device_id_type=MESH,
        )

    def n_copy(way, hop, c):
        return spread(way, hop, c, quarter, n_send, n_recv, sides[pieces[c][1]])

    def p_copy(way, hop, c):
        return spread(way, hop, c, quarter, p_send, p_recv, partner)

    def m_copy(way, hop, c):
        return spread(way, hop, c, across, m_send, m_recv, partner)

    def each_way(hop, act):
        for way in range(2):
            pl.when(inside(origin(way, hop)))(functools.partial(act, way))

    done = set()

    def once(*key):
        fresh = key[1] < depth and key not in done
        done.add(key)
        return fresh

    def z_event(hop, c):
        if not once("z", hop, c):
            return
        each_way(hop, lambda way: z_arrival(way, hop, c).wait_recv())
        if hop + 1 < depth:
            for way in range(2):
                pl.when(sends(way, hop + 1))(lambda way=way: z_copy(way, hop + 1, c).start())

    def s_event(hop, c):
        if not once("s", hop, c):
            return

        def act(way):
            n_copy(way, hop, c).start()
            p_copy(way, hop, c).start()

        each_way(hop, act)

    def n_event(hop, c):
        if not once("n", hop, c):
            return

        def act(way):
            n_copy(way, hop, c).wait_recv()
            m_copy(way, hop, c).start()

        each_way(hop, act)

    def f_event(hop):
        if not once("f", hop):
            return
        for event in (z_event, s_event, n_event):
            for c in range(len(pieces)):
                event(hop, c)

        def act(way):
            for c in range(len(pieces)):
                p_copy(way, hop, c).wait_recv()
                m_copy(way, hop, c).wait_recv()

        each_way(hop, act)

    def w_end():
        for hop in range(1, depth):
            f_event(hop)
        for hop in range(1, depth):
            for way in range(2):
                for c in range(len(pieces)):
                    pl.when(sends(way, hop))(
                        lambda way=way, hop=hop, c=c: z_copy(way, hop, c).wait_send()
                    )

            def act(way, hop=hop):
                for c in range(len(pieces)):
                    for make in (n_copy, p_copy, m_copy):
                        make(way, hop, c).wait_send()

            each_way(hop, act)

    for c in range(len(pieces)):
        for way in range(2):
            pl.when(sends(way, 1))(lambda way=way, c=c: z_copy(way, 1, c).start())

    def c_copy(b):
        return pltpu.make_async_remote_copy(
            src_ref=total.at[b, pl.ds((1 - core) * held, held)], dst_ref=core_in.at[b],
            send_sem=c_send.at[b], recv_sem=c_recv.at[b],
            device_id=partner, device_id_type=MESH,
        )

    def r_copy(b, k):
        return pltpu.make_async_remote_copy(
            src_ref=out_buf.at[b, pl.ds(peer_place(k) * piece, piece)],
            dst_ref=in_buf.at[b, k - 1],
            send_sem=r_send.at[b, k], recv_sem=r_recv.at[b, k],
            device_id=peers[k - 1], device_id_type=MESH,
        )

    def g_copy(b, k):
        at = final.at[b, pl.ds(core * held + place * piece, piece)]
        return pltpu.make_async_remote_copy(
            src_ref=at, dst_ref=at, send_sem=g_send.at[b, k], recv_sem=g_recv.at[b, k],
            device_id=peers[k - 1], device_id_type=MESH,
        )

    def f_copy(b):
        at = final.at[b, pl.ds(core * held, held)]
        return pltpu.make_async_remote_copy(
            src_ref=at, dst_ref=at, send_sem=f_send.at[b], recv_sem=f_recv.at[b],
            device_id=partner, device_id_type=MESH,
        )

    def x_add(b):
        c_copy(b).wait()
        mine = pl.ds(core * held, held)
        summed = total[b, mine] + core_in[b]
        total[b, mine] = summed
        out_buf[b, :, :size] = summed[:, :size].astype(bf16)
        out_buf[b, :, size:] = split_mass(summed[:, size:])
        for k in range(1, places):
            r_copy(b, k).start()

    def x_sum(b):
        mine = pl.ds(core * held + place * piece, piece)
        state, mass = total[b, mine, :size], total[b, mine, size:]
        for k in range(1, places):
            r_copy(b, k).wait_recv()
            state += in_buf[b, k - 1, :, :size].astype(f32)
            pair = in_buf[b, k - 1, :, size:].astype(f32)
            mass += pair[:, :1] + pair[:, 1:2]
        final[b, mine, :size] = (state / count).astype(bf16)
        final[b, mine, size:] = split_mass(mass / count / root)
        for k in range(1, places):
            g_copy(b, k).start()

    def x_share(b):
        for k in range(1, places):
            g_copy(b, k).wait_recv()
        f_copy(b).start()

    def x_table(b):
        f_copy(b).wait_recv()
        for h in range(heads):
            pair = final[b, h, size:].astype(f32)
            table[h, :size, :size] = final[b, h, :size]
            table[h, size:, :size] = jnp.broadcast_to(pair[:1], (size, size)).astype(bf16)
            table[h, size:, size:] = jnp.broadcast_to(pair[1:2], (size, size)).astype(bf16)

    def x_end(b):
        for k in range(1, places):
            r_copy(b, k).wait_send()
            g_copy(b, k).wait_send()
        f_copy(b).wait_send()

    groups_of = tile // GROUP

    def regroup(g, values, store):
        region = regions[g % REGIONS]
        for part_of in range(heads // SUBLANES):
            start = part_of * SUBLANES
            region.at[part_of].reshape(GROUP, SUBLANES, size)[...] = values[
                :, start : start + SUBLANES
            ]
        for h in range(heads):
            line = pl.ds(h % SUBLANES, GROUP, stride=SUBLANES)
            store(h, region[h // SUBLANES, line, :].astype(bf16))

    ones = jnp.ones((EXTRA, tile), bf16)

    def fold(i):
        slot, b = i % SLOTS, i // per_batch
        rel_k.reshape(tile, PITCH, size)[:, :heads, :] = feature_map(k_buf[slot])
        v_heads = pltpu.einshape("thd->htd", v_buf[slot])
        for h in range(heads):
            left = jnp.concatenate([jnp.transpose(v_heads[h]), ones], axis=0)
            right = rel_k[pl.ds(h, tile, stride=PITCH), :].astype(bf16)
            total[b, h] += jnp.dot(left, right, preferred_element_type=f32)

    def spot(i, h):
        block_of, column = divmod(h * size, rows)
        return block_of, pl.ds(i * tile, tile), pl.ds(column, size)

    def prepare(i):
        for g in range(groups_of):
            def put(h, x, g=g):
                block_of, column = divmod(h * size, rows)
                at = pl.ds(i * tile + g * GROUP, GROUP)
                mixed[block_of, at, pl.ds(column, size)] = x

            regroup(g, feature_map(q_buf[i % SLOTS, pl.ds(g * GROUP, GROUP)]), put)

    def read(i):
        for h in range(heads):
            feature = mixed[spot(i, h)]
            both = lax.dot_general(
                jnp.concatenate([feature, feature], axis=1), table[h],
                (((1,), (1,)), ((), ())), preferred_element_type=f32,
            )
            top = both[:, :size] / (both[:, size:] + 0.001 / root)
            mixed[spot(i, h)] = top.astype(bf16)

    broad = min(2 * tile, tokens)

    def project(i, j):
        at, source = pl.ds(i * broad, broad), nearest(d, depth, j)
        product = jnp.dot(mixed[source, at], w_all[source], preferred_element_type=f32)
        acc[at, :] = product if j == 0 else acc[at, :] + product

    def at_step(i, events):
        for moment, items in events.items():
            if not items:
                continue

            def run(items=items):
                for item in items:
                    item()

            pl.when(i == moment)(run)

    def make(function, *args):
        return functools.partial(function, *args)

    plan, clock = [], [T_FOLD]

    def due():
        now = []
        while plan and plan[0][0] <= clock[0]:
            now.append(plan.pop(0)[1])
        return now

    def run_due():
        for event in due():
            event()

    def loop(start, stop, body, length, extra=None):
        events = {}
        for i in range(start, stop):
            events[i] = (extra or {}).get(i, []) + due()
            clock[0] += length

        def one(i, carry):
            at_step(i, events)
            body(i)
            return carry

        lax.fori_loop(start, stop, one, 0)

    def fold_step(i):
        @pl.when(i + SLOTS - 1 < steps)
        def _():
            for copy in load(i + SLOTS - 1):
                copy.start()

        @pl.when(i + SLOTS - 1 >= steps)
        def _():
            load_q(i + SLOTS - 1 - steps).start()

        for copy in load(i):
            copy.wait()
        fold(i)

    def prepare_step(i):
        @pl.when(i + SLOTS - 1 < steps)
        def _():
            load_q(i + SLOTS - 1).start()

        load_q(i).wait()
        prepare(i)

    half = per_batch
    t_half = T_FOLD + half * D_FOLD
    t_full = T_FOLD + steps * D_FOLD
    free = [0.0, 0.0]
    for hop in range(1, depth):
        for c in range(len(pieces)):
            arrival = T_Z + D_Z * (len(pieces) * (hop - 1) + c + 1)
            ready, side = max(arrival, HOLD), pieces[c][1]
            free[side] = max(free[side], ready) + D_Z * (2 if hop == 1 else 1)
            plan.append((arrival, make(z_event, hop, c)))
            plan.append((ready, make(s_event, hop, c)))
            plan.append((free[side] + D_N, make(n_event, hop, c)))
    plan.append((t_half + D_C, make(x_add, 0)))
    plan.append((t_half + D_C + D_R, make(x_sum, 0)))
    plan.append((t_half + D_C + D_R + D_G, make(x_share, 0)))
    plan.append((t_full + D_C, make(x_add, 1)))
    plan.append((t_full + D_C + D_R, make(x_sum, 1)))
    plan.append((t_full + D_C + D_R + D_G, make(x_share, 1)))
    plan.sort(key=lambda item: item[0])

    def require(name, b):
        for index, item in enumerate(plan):
            if item[1].func is name and item[1].args == (b,):
                for _ in range(index + 1):
                    plan.pop(0)[1]()
                clock[0] = max(clock[0], item[0])
                return

    loop(0, steps, fold_step, D_FOLD, {half: [lambda: c_copy(0).start()]})
    c_copy(1).start()
    loop(0, steps, prepare_step, D_PREPARE)
    own.wait()
    require(x_share, 0)
    run_due()
    x_table(0)
    clock[0] += D_TABLE
    loop(0, half, read, D_READ)
    mid = half * tile // broad
    end = 2 * mid
    loop(0, mid, lambda i: project(i, 0), D_PROJECT)
    require(x_share, 1)
    run_due()
    x_table(1)
    clock[0] += D_TABLE
    loop(half, steps, read, D_READ)
    loop(mid, end, lambda i: project(i, 0), D_PROJECT)
    for j in range(1, depth - 1):
        f_event(j)
        loop(0, end, lambda i, j=j: project(i, j), D_PROJECT)
    for b in range(batch):
        x_end(b)
    w_end()


def nearest(d, depth, j):
    both = 2 * jnp.minimum(d, depth - 1 - d)
    around = d - (j + 1) // 2 if j % 2 else d + j // 2
    return jnp.where(j <= both, around, jnp.where(d < depth - 1 - d, j, depth - 1 - j))


def close_kernel(depth, tile, acc, mixed, w_all, out_ref, stage, sem):
    source = nearest(lax.axis_index("dp"), depth, depth - 1)
    steps = acc.shape[0] // tile

    def store(i):
        return pltpu.make_async_copy(
            stage.at[i % 2], out_ref.at[pl.ds(i * tile, tile)], sem.at[i % 2]
        )

    def step(i, carry):
        at = pl.ds(i * tile, tile)
        pl.when(i > 1)(lambda: store(i - 2).wait())
        product = jnp.dot(mixed[source, at], w_all[source], preferred_element_type=jnp.float32)
        stage[i % 2] = (acc[at, :] + product).astype(jnp.bfloat16)
        store(i).start()
        return carry

    lax.fori_loop(0, steps, step, 0)
    for i in range(max(steps - 2, 0), steps):
        store(i).wait()


def close(acc, mixed, w_all, tile):
    vmem = pl.BlockSpec(memory_space=pltpu.VMEM)
    total, width = acc.shape
    return pl.pallas_call(
        functools.partial(close_kernel, w_all.shape[0], tile),
        out_shape=jax.ShapeDtypeStruct((total, width), jnp.bfloat16),
        in_specs=[vmem] * 3,
        out_specs=pl.BlockSpec(memory_space=pl.ANY),
        scratch_shapes=[
            pltpu.VMEM((2, tile, width), jnp.bfloat16),
            pltpu.SemaphoreType.DMA((2,)),
        ],
        compiler_params=pltpu.CompilerParams(vmem_limit_bytes=8 * 2**20),
    )(acc, mixed, w_all)


def gather(queries, keys_in, values_in, out_weight, count):
    batch, tokens, heads, size = keys_in.shape
    depth, lanes = lax.axis_size("dp"), lax.axis_size("sp")
    places = lanes // 2
    rows, width = out_weight.shape
    held, deep = heads // 2, size + EXTRA
    tile = min(TILE, tokens)
    any_space = pl.BlockSpec(memory_space=pl.ANY)
    dma = pltpu.SemaphoreType.DMA
    f32, bf16 = jnp.float32, jnp.bfloat16
    w_dma = dma((2, depth, 2 * CUTS))
    vmem = pl.BlockSpec(memory_space=pltpu.VMEM)
    return pl.pallas_call(
        functools.partial(
            gather_kernel, (depth, lanes), count, tile, batch, tokens, heads, size
        ),
        out_shape=(
            pltpu.VMEM((depth, batch * tokens, rows), bf16),
            pltpu.VMEM((depth, rows, width), bf16),
            pltpu.VMEM((batch * tokens, width), f32),
        ),
        in_specs=[any_space] * 4,
        out_specs=(vmem, vmem, vmem),
        scratch_shapes=[
            pltpu.VMEM((SLOTS, tile, heads, size), bf16),
            pltpu.VMEM((SLOTS, tile, heads, size), bf16),
            pltpu.VMEM((SLOTS, tile, heads, size), bf16),
            [pltpu.VMEM((heads // SUBLANES, GROUP * SUBLANES, size), f32)] * REGIONS,
            pltpu.VMEM((tile * PITCH, size), f32),
            pltpu.VMEM((batch, heads, deep, size), f32),
            pltpu.VMEM((batch, held, deep, size), f32),
            pltpu.VMEM((batch, held, deep, size), bf16),
            pltpu.VMEM((batch, places - 1, held // places, deep, size), bf16),
            pltpu.VMEM((batch, heads, deep, size), bf16),
            pltpu.VMEM((heads, 2 * size, 2 * size), bf16),
            dma((2, SLOTS)),
            dma((SLOTS,)),
            dma,
            w_dma, w_dma, w_dma, w_dma, w_dma, w_dma, w_dma, w_dma,
            dma((batch,)),
            dma((batch,)),
            dma((batch, places)),
            dma((batch, places)),
            dma((batch, places)),
            dma((batch, places)),
            dma((batch,)),
            dma((batch,)),
        ],
        compiler_params=pltpu.CompilerParams(
            collective_id=0, has_side_effects=True, vmem_limit_bytes=26 * 2**20
        ),
    )(queries, keys_in, values_in, out_weight)


def on_device(queries_in, keys_in, values_in, out_weight):
    batch, tokens = queries_in.shape[:2]
    count = tokens * lax.axis_size("sp")
    mixed, w_all, acc = gather(queries_in, keys_in, values_in, out_weight, count)
    out = close(acc, mixed, w_all, min(2 * TILE, tokens))
    return out.reshape(batch, tokens, out_weight.shape[1])


def solution(mesh):
    placed = (
        P("dp", "sp", None, None),
        P("dp", "sp", None, None),
        P("dp", "sp", None, None),
        P("dp", None),
    )
    return jax.shard_map(
        on_device, mesh=mesh, in_specs=placed, out_specs=P("dp", "sp", None), check_vma=False
    )
```
